32 devices in a mesh: dp: 4 (over z), expert: 4 (over y, x), tensor: 2 (over core).
Axes of the slice: x: 2, y: 2, z: 4, core: 2. Of those that a mesh axis runs over, the one named last changes fastest.
Arguments:
- tokens: bfloat16 [1536, 3072], P(('dp', 'expert', 'tensor')), may hold values from -6 to 6
- grad_out: bfloat16 [1536, 3072], P(('dp', 'expert', 'tensor')), may hold values from -3 to 3
- gates: float32 [1536, 2], P(('dp', 'expert', 'tensor')), may hold values from 0.1 to 0.9
- expert_ids: int32 [1536, 2], P(('dp', 'expert')), may hold values from 0 to 3, all different within a row
- w_gate: bfloat16 [4, 3072, 8192], P('expert', None, ('dp', 'tensor')), may hold values from -0.109375 to 0.109375
- w_up: bfloat16 [4, 3072, 8192], P('expert', None, ('dp', 'tensor')), may hold values from -0.109375 to 0.109375
- w_down: bfloat16 [4, 3072, 8192], P('expert', None, ('dp', 'tensor')), may hold values from -0.0625 to 0.0625
Outputs:
- grad_tokens: bfloat16 [1536, 3072], P(('dp', 'expert', 'tensor'))
- grad_gate: bfloat16 [4, 3072, 8192], P('expert', None, ('dp', 'tensor'))
- grad_up: bfloat16 [4, 3072, 8192], P('expert', None, ('dp', 'tensor'))
- grad_down: bfloat16 [4, 3072, 8192], P('expert', None, ('dp', 'tensor'))
The draws below stay inside these ranges and needn't reach their ends.
Inputs may be any that keep to these rules, and one draw needn't show every extreme that they name: `expert_ids`: each token names 2 different experts, and every expert is named by some token.
All inputs are finite; a program needn't handle non-finite values.
Results may differ from the reference program's by a relative error of at most 0.017.
Values may be sent and summed in bfloat16 or wider, within the bound.
A program may use at most 128 MiB of HBM per device.

```python
import jax
import jax.numpy as jnp
from jax import lax

D = 3072
FF = 8192
TOP = 2
TOK_GRP = 96
EXPERTS = 4
CAP = 60
TOKENS = 1536


def shard_levels(key, dims, split, low, largest):
    gain = 1.0
    for dim, parts in split:
        heights = jax.random.uniform(jax.random.fold_in(jax.random.fold_in(key, 6), dim), (parts,), jnp.float32, low / len(split), largest / len(split))
        gain = gain * jnp.repeat(jnp.exp(heights), dims[dim] // parts).reshape((-1,) + (1,) * (len(dims) - 1 - dim))
    return gain


def different_ones(rng, rows, amount, top, lift):
    sequence = jax.random.permutation(jax.random.fold_in(rng, 1), amount)
    pull = sequence
    for power in range(3):
        pull = pull * pull // amount
    pull = pull * lift // amount
    tickets = jax.random.randint(jax.random.fold_in(rng, 2), (rows, amount), 0, 4096) + pull
    holders = jax.random.permutation(jax.random.fold_in(rng, 3), rows)[jnp.arange(amount) % rows]
    tickets = jnp.where(jnp.arange(rows)[:, None] == holders[None, :], 1 << 14, tickets)
    score = tickets * amount + jnp.arange(amount)
    return lax.top_k(score.astype(jnp.int32), top)[1].astype(jnp.int32)


def centred(key, shape, width, limit, pieces=(), kind=jnp.bfloat16):
    array = width * jax.random.normal(key, shape, jnp.float32)
    if pieces:
        array = array * shard_levels(key, shape, pieces, -0.22, 0.18)
    return jnp.clip(array, -limit, limit).astype(kind)


def setup_inputs(seed: int = 0) -> dict:
    splits = jax.random.split(jax.random.key(seed), 8)
    return {
        "tokens": centred(splits[0], (TOKENS, D), 1.0, 6.0, ((0, 32),)),
        "grad_out": centred(splits[1], (TOKENS, D), 0.5, 3.0, ((0, 32),)),
        "gates": jnp.clip(0.1 + 0.79999997 * jax.random.uniform(splits[2], (TOKENS, TOP), jnp.float32) ** shard_levels(splits[2], (TOKENS, TOP), ((0, 32),), -0.2, 0.2), 0.1, 0.9),
        "expert_ids": different_ones(splits[3], TOKENS, EXPERTS, TOP, 8192),
        "w_gate": centred(splits[4], (EXPERTS, D, FF), D ** -0.5, 0.109375, ((0, 4), (2, 8))),
        "w_up": centred(splits[5], (EXPERTS, D, FF), D ** -0.5, 0.109375, ((0, 4), (2, 8))),
        "w_down": centred(splits[6], (EXPERTS, D, FF), FF ** -0.5, 0.0625, ((0, 4), (2, 8))),
    }


def dispatch_table(expert_ids):
    id_blocks = expert_ids.reshape(-1, TOK_GRP * TOP)
    onehot = (id_blocks[:, :, None] == jnp.arange(EXPERTS, dtype=jnp.int32)[None, None, :]).astype(jnp.int32)
    before = jnp.cumsum(onehot, axis=1) - onehot
    slot_index = jnp.sum(before * onehot, axis=2)
    target = jnp.where(slot_index < CAP, id_blocks * CAP + slot_index, EXPERTS * CAP)
    slot_table = target[:, :, None] == jnp.arange(EXPERTS * CAP, dtype=jnp.int32)[None, None, :]
    return slot_table.astype(jnp.float32)


def reference(tokens, grad_out, gates, expert_ids, w_gate, w_up, w_down):
    block_count = TOKENS // TOK_GRP
    slot_table = dispatch_table(expert_ids)
    rows_x = jnp.repeat(tokens.reshape(block_count, TOK_GRP, D), TOP, axis=1).astype(jnp.float32)
    scaled = gates.reshape(block_count, TOK_GRP * TOP, 1) * jnp.repeat(grad_out.reshape(block_count, TOK_GRP, D), TOP, axis=1).astype(jnp.float32)
    gated_rows = scaled.astype(jnp.bfloat16).astype(jnp.float32)
    x_buffer = jnp.einsum('bae,bad->bed', slot_table, rows_x).astype(jnp.bfloat16).reshape(block_count, EXPERTS, CAP, D)
    g_buffer = jnp.einsum('bae,bad->bed', slot_table, gated_rows).astype(jnp.bfloat16).reshape(block_count, EXPERTS, CAP, D)
    grads_gate, grads_up, grads_down, slot_list = [], [], [], []
    for expert in range(EXPERTS):
        slot_x = x_buffer[:, expert].reshape(block_count * CAP, D)
        slot_g = g_buffer[:, expert].reshape(block_count * CAP, D)
        h_gate = jnp.dot(slot_x, w_gate[expert], preferred_element_type=jnp.float32)
        h_up = jnp.dot(slot_x, w_up[expert], preferred_element_type=jnp.float32)
        d_act = jnp.dot(slot_g, w_down[expert], preferred_element_type=jnp.float32)
        sigmoid_gate = jax.nn.sigmoid(h_gate)
        activated = (h_gate * sigmoid_gate * h_up).astype(jnp.bfloat16)
        d_up = (d_act * h_gate * sigmoid_gate).astype(jnp.bfloat16)
        d_gate = (d_act * h_up * sigmoid_gate * (1.0 + h_gate * (1.0 - sigmoid_gate))).astype(jnp.bfloat16)
        grads_gate.append(jnp.dot(slot_x.T, d_gate, preferred_element_type=jnp.float32).astype(jnp.bfloat16))
        grads_up.append(jnp.dot(slot_x.T, d_up, preferred_element_type=jnp.float32).astype(jnp.bfloat16))
        grads_down.append(jnp.dot(slot_g.T, activated, preferred_element_type=jnp.float32).astype(jnp.bfloat16))
        backward = jnp.dot(d_gate, w_gate[expert].T, preferred_element_type=jnp.float32)
        backward = backward + jnp.dot(d_up, w_up[expert].T, preferred_element_type=jnp.float32)
        slot_list.append(backward.astype(jnp.bfloat16).reshape(block_count, CAP, D))
    slot_grads = jnp.stack(slot_list, axis=1).reshape(block_count, EXPERTS * CAP, D).astype(jnp.float32)
    per_assign = jnp.einsum('bae,bed->bad', slot_table, slot_grads)
    grad_tokens = jnp.sum(per_assign.reshape(block_count, TOK_GRP, TOP, D), axis=2).reshape(TOKENS, D).astype(jnp.bfloat16)
    return grad_tokens, jnp.stack(grads_gate), jnp.stack(grads_up), jnp.stack(grads_down)
```

```python
import jax
import jax.numpy as jnp
from jax import lax
from jax.sharding import PartitionSpec as P

TOP = 2


def shifted(value, axis, amount):
    size = lax.axis_size(axis)
    return lax.ppermute(value, axis, [(i, (i + amount) % size) for i in range(size)])


def exchanged(value, step):
    size = lax.axis_size("expert")
    return lax.ppermute(value, "expert", [(i, i ^ step) for i in range(size)])


def transposed_product(left, right):
    return lax.dot_general(
        left, right, (((0,), (0,)), ((), ())), preferred_element_type=jnp.float32
    )


def product_transposed(left, right):
    return lax.dot_general(
        left, right, (((1,), (1,)), ((), ())), preferred_element_type=jnp.float32
    )


def gather_columns(part):
    members = lax.axis_size("tensor")
    member = lax.axis_index("tensor")
    parts = [part] + [shifted(part, "tensor", m) for m in range(1, members)]
    ordered = []
    for place in range(members):
        piece = parts[0]
        for m in range(1, members):
            piece = jnp.where(lax.rem(member - m + members, members) == place, parts[m], piece)
        ordered.append(piece)
    return jnp.concatenate(ordered, axis=1)


def reduce_columns(whole):
    members = lax.axis_size("tensor")
    member = lax.axis_index("tensor")
    width = whole.shape[1] // members

    def share(m):
        owner = lax.rem(member + m, members)
        return lax.dynamic_slice_in_dim(whole, owner * width, width, 1)

    total = share(0).astype(jnp.float32)
    for m in range(1, members):
        total = total + shifted(share(m), "tensor", m).astype(jnp.float32)
    return total.astype(jnp.bfloat16)


def slot_tables(ids, gates, capacity, experts):
    blocks, group, _ = ids.shape
    own = lax.axis_index("expert")
    flat = ids.reshape(blocks, group * TOP)
    onehot = flat[:, :, None] == jnp.arange(experts, dtype=jnp.int32)[None, None, :]
    place = jnp.arange(group * TOP, dtype=jnp.int32)
    earlier = (place[None, :] < place[:, None]).astype(jnp.bfloat16)
    before = jnp.einsum(
        "ab,kbe->kae", earlier, onehot.astype(jnp.bfloat16), preferred_element_type=jnp.float32
    )
    slot_index = jnp.sum(jnp.where(onehot, before, 0.0), axis=2).astype(jnp.int32)
    block = jnp.arange(blocks, dtype=jnp.int32)[:, None]
    row = (flat ^ own) * (blocks * capacity) + block * capacity + slot_index
    row = jnp.where(slot_index < capacity, row, -1).reshape(blocks * group, TOP)
    gate = gates.reshape(blocks * group, TOP)
    rows = jnp.arange(experts * blocks * capacity, dtype=jnp.int32)[:, None]
    taken = jnp.zeros((rows.shape[0], blocks * group), jnp.bool_)
    slot_gate = jnp.zeros((rows.shape[0],), jnp.float32)
    for k in range(TOP):
        match = rows == row[:, k][None, :]
        taken = taken | match
        slot_gate = slot_gate + jnp.sum(jnp.where(match, gate[:, k][None, :], 0.0), axis=1)
    return taken.astype(jnp.bfloat16), slot_gate[:, None]


def dispatch(slots, experts):
    part = slots.shape[0] // experts
    pieces = [slots[:part]]
    for step in range(1, experts):
        pieces.append(exchanged(slots[step * part : (step + 1) * part], step))
    return gather_columns(jnp.concatenate(pieces, axis=0))


def local(tokens, grad_out, gates, expert_ids, w_gate, w_up, w_down):
    experts = w_gate.shape[0] * lax.axis_size("expert")
    members = lax.axis_size("tensor")
    member = lax.axis_index("tensor")
    planes = lax.axis_size("dp")
    plane = lax.axis_index("dp")
    own_rows = tokens.shape[0]
    group = own_rows * members
    capacity = (5 * group * TOP + 4 * experts * members - 1) // (4 * experts * members) * members
    gate_w, up_w, down_w = w_gate[0], w_up[0], w_down[0]

    own_ids = lax.dynamic_slice_in_dim(expert_ids, member * own_rows, own_rows, 0)
    packed = jnp.concatenate([gates, own_ids.astype(jnp.float32)], axis=1)
    packed = lax.all_gather(packed, ("dp", "tensor"), axis=0, tiled=True)
    packed = packed.reshape(planes, group, 2 * TOP)

    packed, tokens, grad_out = lax.optimization_barrier((packed, tokens, grad_out))
    x_own = lax.all_to_all(tokens, "tensor", split_axis=1, concat_axis=0, tiled=True)
    c_own = lax.all_to_all(grad_out, "tensor", split_axis=1, concat_axis=0, tiled=True)
    x_planes = [x_own] + [shifted(x_own, "dp", k) for k in range(1, planes)]
    c_own, _ = lax.optimization_barrier((c_own, x_planes[-1]))
    c_planes = [c_own] + [shifted(c_own, "dp", k) for k in range(1, planes)]

    half = max(planes // 2, 1)
    chunks = [list(range(lo, min(lo + half, planes))) for lo in range(0, planes, half)]
    tables, slot_x, slot_g = [], [], []
    for chunk in chunks:
        info = jnp.stack(
            [
                lax.dynamic_index_in_dim(packed, lax.rem(plane - k + planes, planes), 0, False)
                for k in chunk
            ]
        )
        tables.append(
            slot_tables(info[:, :, TOP:].astype(jnp.int32), info[:, :, :TOP], capacity, experts)
        )
    for chunk, (taken, _) in zip(chunks, tables):
        rows = jnp.concatenate([x_planes[k] for k in chunk], axis=0)
        slots = jnp.dot(taken, rows, preferred_element_type=jnp.float32).astype(jnp.bfloat16)
        slot_x.append(dispatch(slots, experts))
    for place, (chunk, (taken, slot_gate)) in enumerate(zip(chunks, tables)):
        rows = jnp.concatenate([c_planes[k] for k in chunk], axis=0)
        slots = jnp.dot(taken, rows, preferred_element_type=jnp.float32)
        slots = (slots * slot_gate).astype(jnp.bfloat16)
        slots, slot_x[place] = lax.optimization_barrier((slots, slot_x[place]))
        slot_g.append(dispatch(slots, experts))

    hidden = [
        (
            jnp.dot(x, gate_w, preferred_element_type=jnp.float32),
            jnp.dot(x, up_w, preferred_element_type=jnp.float32),
        )
        for x in slot_x
    ]
    acts, d_gates, d_ups, sums = [], [], [], []
    for (h_gate, h_up), g in zip(hidden, slot_g):
        d_act = jnp.dot(g, down_w, preferred_element_type=jnp.float32)
        sig = jax.nn.sigmoid(h_gate)
        acts.append((h_gate * sig * h_up).astype(jnp.bfloat16))
        d_ups.append((d_act * h_gate * sig).astype(jnp.bfloat16))
        d_gates.append((d_act * h_up * sig * (1.0 + h_gate * (1.0 - sig))).astype(jnp.bfloat16))

    token_sum, marks = None, []
    for chunk, (taken, _), d_gate, d_up in zip(chunks, tables, d_gates, d_ups):
        backward = product_transposed(d_gate, gate_w) + product_transposed(d_up, up_w)
        backward = backward.astype(jnp.bfloat16)
        marks.append(backward)
        backward = reduce_columns(backward)
        marks.append(backward)
        part = backward.shape[0] // experts
        pieces = [backward[:part]]
        for step in range(1, experts):
            pieces.append(exchanged(backward[step * part : (step + 1) * part], step))
        returned = jnp.concatenate(pieces, axis=0)
        terms = transposed_product(taken, returned).astype(jnp.bfloat16)
        for place, k in enumerate(chunk):
            term = terms[place * group : (place + 1) * group]
            if k:
                term = shifted(term, "dp", -k)
            term = term.astype(jnp.float32)
            token_sum = term if token_sum is None else token_sum + term
    grad_tokens = lax.all_to_all(
        token_sum.astype(jnp.bfloat16), "tensor", split_axis=0, concat_axis=1, tiled=True
    )

    all_x, all_g = jnp.concatenate(slot_x, axis=0), jnp.concatenate(slot_g, axis=0)
    all_x, all_g = lax.optimization_barrier((all_x, all_g))

    def weight_grad(rows, parts, mark):
        parts, _ = lax.optimization_barrier((jnp.concatenate(parts, axis=0), mark))
        return transposed_product(rows, parts)

    grad_down = weight_grad(all_g, acts, marks[-2])
    grad_gate = weight_grad(all_x, d_gates, marks[-1])
    grad_up = weight_grad(all_x, d_ups, marks[-1])
    return (
        grad_tokens,
        grad_gate.astype(jnp.bfloat16)[None],
        grad_up.astype(jnp.bfloat16)[None],
        grad_down.astype(jnp.bfloat16)[None],
    )


def solution(mesh):
    in_specs = (
        P(("dp", "expert", "tensor"), None),
        P(("dp", "expert", "tensor"), None),
        P(("dp", "expert", "tensor"), None),
        P(("dp", "expert"), None),
        P("expert", None, ("dp", "tensor")),
        P("expert", None, ("dp", "tensor")),
        P("expert", None, ("dp", "tensor")),
    )
    out_specs = (
        P(("dp", "expert", "tensor"), None),
        P("expert", None, ("dp", "tensor")),
        P("expert", None, ("dp", "tensor")),
        P("expert", None, ("dp", "tensor")),
    )
    return jax.shard_map(local, mesh=mesh, in_specs=in_specs, out_specs=out_specs, check_vma=False)
```
